32 devices in a mesh: len: 2 (over x), tile: 16 (over z, y, core).
Axes of the slice: x: 2, y: 2, z: 4, core: 2. Of those that a mesh axis runs over, the one named last changes fastest.
Arguments:
- series: float32 [9216], P('tile'), may hold values from -24 to 24
- window_lengths: int32 [4], P('len'), may hold values from 64 to 1024, as said below
- exclusion: int32 [4], P('len'), may hold values from 16 to 256
- tile_list: int32 [64, 2], P('tile'), may hold values from 0 to 15, as said below
Outputs:
- right_profile: float32 [4, 8192], P(None, 'tile')
- left_profile: float32 [4, 8192], P(None, 'tile')
The draws below stay inside these ranges and needn't reach their ends.
Inputs may be any that keep to these rules, and one draw needn't show every extreme that they name: `window_lengths`: the largest is exactly 1024. `tile_list`: each row is a pair (row block, column block) with row block <= column block; no pair appears twice.
All inputs are finite; a program needn't handle non-finite values.
Results may differ from the reference program's by a relative error of at most 0.00039.
Values sent between devices are 32-bit elements; how exact they have to be, the bound alone decides.
No kernel may reach another device: no remote copies, remote signals or barrier semaphores. Data moves between devices by JAX's collectives and lax.ppermute only.
A program may use at most 64 MiB of HBM per device.

```python
import jax
import jax.numpy as jnp
from jax import lax

MIN_LEN = 64
OCTAVES = 4
MAX_LEN = 1024
LENGTHS = 4
TILE_SIDE = 512
COL_BLOCK = 512
TILE_ROWS = 16
SERIES_LENGTH = 9216
TILE_SLOTS = 64


def draw_series(key, part):
    noise_key, wave_key, phase_key = jax.random.split(key, 3)
    sample_times = jnp.arange(SERIES_LENGTH, dtype=jnp.float32)
    wave_frequencies = jax.random.uniform(wave_key, (4,), jnp.float32, 0.002, 0.05)
    wave_phases = jax.random.uniform(phase_key, (4,), jnp.float32, -3.14159, 3.14159)
    smoothed_series = 0.5 * jnp.sum(jnp.sin(sample_times[:, None] * wave_frequencies[None, :] + wave_phases[None, :]), axis=1)
    jitter = jnp.clip(jax.random.normal(noise_key, (SERIES_LENGTH,), jnp.float32), -6.0, 6.0)
    return jitter + smoothed_series


def draw_window_lengths(key, part):
    octave_key, offset_key, pick_key = jax.random.split(key, 3)
    octave = jax.random.randint(octave_key, (LENGTHS,), 0, OCTAVES)
    lowest = MIN_LEN * jnp.left_shift(jnp.ones((LENGTHS,), jnp.int32), octave.astype(jnp.int32))
    surplus = jax.random.randint(offset_key, (LENGTHS,), 0, 1 << 30) % (lowest + 1)
    chosen = jax.random.randint(pick_key, (), 0, LENGTHS)
    lengths = jnp.where(jnp.arange(LENGTHS) == chosen, MAX_LEN, lowest + surplus)
    return lengths.astype(jnp.int32)


def draw_tile_list(key, part):
    grid_rows = lax.broadcasted_iota(jnp.int32, (TILE_ROWS, TILE_ROWS), 0)
    grid_cols = lax.broadcasted_iota(jnp.int32, (TILE_ROWS, TILE_ROWS), 1)
    upper = (grid_rows <= grid_cols).reshape(-1)
    triangle = TILE_ROWS * (TILE_ROWS + 1) // 2
    flat_ids = jnp.nonzero(upper, size=triangle)[0].astype(jnp.int32)
    order = jax.random.permutation(key, triangle)[:TILE_SLOTS]
    picked = flat_ids[order]
    return jnp.stack([picked // TILE_ROWS, picked % TILE_ROWS], axis=1).astype(jnp.int32)


def place_ends(result, stream_key, low, largest):
    spot = [jax.random.randint(jax.random.fold_in(stream_key, axis), (), 0, length) for axis, length in enumerate(result.shape)]
    longest = result.shape.index(max(result.shape))
    neighbour = spot[:longest] + [(spot[longest] + 1) % result.shape[longest]] + spot[longest + 1:]
    return result.at[tuple(spot)].set(low).at[tuple(neighbour)].set(largest)


def setup_inputs(seed: int = 0) -> dict:
    keys = jax.random.split(jax.random.key(seed), 5)
    series = draw_series(jax.random.fold_in(keys[4], 71), 0)
    window_lengths = draw_window_lengths(jax.random.fold_in(keys[4], 71), 0)
    exclusion = place_ends(jax.random.randint(keys[2], (LENGTHS,), MIN_LEN // 4, MAX_LEN // 4 + 1), jax.random.fold_in(keys[2], 1), MIN_LEN // 4, (MAX_LEN // 4 + 1) - 1).astype(jnp.int32)
    tile_list = draw_tile_list(jax.random.fold_in(keys[4], 71), 0)
    return {"series": series, "window_lengths": window_lengths, "exclusion": exclusion, "tile_list": tile_list}


EMPTY_VALUE = 2.0
VAR_EPS = 1e-05

def shifted_block(segment, offset, columns, positions):
    window = lax.dynamic_slice_in_dim(segment, offset, positions + columns)
    stride = positions + columns + 1
    repeated = jnp.tile(window, columns + 1)[:columns * stride]
    return repeated.reshape(columns, stride)[:, :positions]

def window_stats(segment, length, positions, columns):
    blocks = (length + columns - 1) // columns
    col_ids = lax.broadcasted_iota(jnp.int32, (columns, 1), 0)
    denominator = length.astype(jnp.float32)
    initial = jnp.zeros((positions,), jnp.float32)

    def add_sum(part_index, running):
        values = shifted_block(segment, part_index * columns, columns, positions)
        inside = col_ids + part_index * columns < length
        return running + lax.optimization_barrier(jnp.sum(jnp.where(inside, values, 0.0), axis=0))
    centre = lax.fori_loop(0, blocks, add_sum, initial) / denominator

    def add_square(part_index, running):
        values = shifted_block(segment, part_index * columns, columns, positions) - centre[None, :]
        inside = col_ids + part_index * columns < length
        return running + lax.optimization_barrier(jnp.sum(jnp.where(inside, values * values, 0.0), axis=0))
    spread = lax.fori_loop(0, blocks, add_square, initial) / denominator
    return (centre, 1.0 / jnp.sqrt(spread + VAR_EPS))

def normalized(segment, part_index, centre, inverse, length):
    values = shifted_block(segment, part_index * COL_BLOCK, COL_BLOCK, TILE_SIDE)
    col_ids = lax.broadcasted_iota(jnp.int32, (COL_BLOCK, 1), 0)
    inside = col_ids + part_index * COL_BLOCK < length
    return jnp.where(inside, (values - centre[None, :]) * inverse[None, :], 0.0).astype(jnp.bfloat16)

def tile_minima(row_segment, col_segment, row_stats, col_stats, length, barrier, row_start, col_start):
    blocks = (length + COL_BLOCK - 1) // COL_BLOCK

    def add_block(part_index, running):
        row_normal = normalized(row_segment, part_index, row_stats[0], row_stats[1], length).astype(jnp.float32)
        col_normal = normalized(col_segment, part_index, col_stats[0], col_stats[1], length).astype(jnp.float32)
        return running + lax.dot_general(row_normal, col_normal, (((0,), (0,)), ((), ())), precision=lax.Precision.HIGHEST, preferred_element_type=jnp.float32)
    product = lax.fori_loop(0, blocks, add_block, jnp.zeros((TILE_SIDE, TILE_SIDE), jnp.float32))
    distance = 1.0 - product / length.astype(jnp.float32)
    row_ids = row_start + lax.broadcasted_iota(jnp.int32, (TILE_SIDE, 1), 0)
    col_ids = col_start + lax.broadcasted_iota(jnp.int32, (1, TILE_SIDE), 1)
    distance = jnp.where(col_ids - row_ids > barrier, distance, EMPTY_VALUE)
    return (lax.optimization_barrier(jnp.min(distance, axis=1)), lax.optimization_barrier(jnp.min(distance, axis=0)))

def reference(series, window_lengths, exclusion, tile_list):
    positions = TILE_ROWS * TILE_SIDE
    block_ids = jnp.arange(TILE_ROWS, dtype=jnp.int32)

    def one_length(setting):
        length, barrier = setting

        def stats_block(row_block):
            segment = lax.dynamic_slice_in_dim(series, row_block * TILE_SIDE, TILE_SIDE + MAX_LEN)
            return window_stats(segment, length, TILE_SIDE, COL_BLOCK)
        centres, inverses = lax.map(stats_block, block_ids)
        centres = centres.reshape(positions)
        inverses = inverses.reshape(positions)

        def one_tile(profiles, tile_pair):
            right_lowest_distance, left_best = profiles
            row_start = (tile_pair[0] * TILE_SIDE).astype(jnp.int32)
            col_start = (tile_pair[1] * TILE_SIDE).astype(jnp.int32)
            row_segment = lax.dynamic_slice_in_dim(series, row_start, TILE_SIDE + MAX_LEN)
            col_segment = lax.dynamic_slice_in_dim(series, col_start, TILE_SIDE + MAX_LEN)
            row_stats = (lax.dynamic_slice_in_dim(centres, row_start, TILE_SIDE), lax.dynamic_slice_in_dim(inverses, row_start, TILE_SIDE))
            col_stats = (lax.dynamic_slice_in_dim(centres, col_start, TILE_SIDE), lax.dynamic_slice_in_dim(inverses, col_start, TILE_SIDE))
            right_min, left_min = tile_minima(row_segment, col_segment, row_stats, col_stats, length, barrier, row_start, col_start)
            right_old = lax.dynamic_slice_in_dim(right_lowest_distance, row_start, TILE_SIDE)
            right_lowest_distance = lax.dynamic_update_slice_in_dim(right_lowest_distance, jnp.minimum(right_old, right_min), row_start, 0)
            left_old = lax.dynamic_slice_in_dim(left_best, col_start, TILE_SIDE)
            left_best = lax.dynamic_update_slice_in_dim(left_best, jnp.minimum(left_old, left_min), col_start, 0)
            return ((right_lowest_distance, left_best), None)
        blank = jnp.full((positions,), EMPTY_VALUE, jnp.float32)
        profiles, leftover = lax.scan(one_tile, (blank, blank), tile_list)
        return profiles
    right_lowest_distance, left_best = lax.map(one_length, (window_lengths, exclusion))
    return (right_lowest_distance, left_best)
```

```python
import functools

import jax
import jax.numpy as jnp
from jax import lax
from jax.experimental import pallas as pl
from jax.experimental.pallas import tpu as pltpu
from jax.sharding import PartitionSpec as P

MAX_LEN = 1024
TILE_SIDE = 512
EMPTY_VALUE = 2.0
VAR_EPS = 1e-05
LANES = 128
CHUNK = 256
LOWEST = -3.0e38
WORD = 16


def round_up(value, multiple):
    return (value + multiple - 1) // multiple * multiple


def packed_piece(series, window_lengths, exclusion, tile_list):
    piece_rows = -(-series.shape[0] // LANES)
    rows = round_up(piece_rows + 3, 8)
    values = jnp.pad(series, (0, piece_rows * LANES - series.shape[0])).reshape(piece_rows, LANES)
    slots = tile_list.astype(jnp.float32).T
    slots = jnp.pad(slots, ((0, 0), (0, LANES - slots.shape[1])), constant_values=-1.0)
    half = LANES // 2
    count = window_lengths.shape[0]
    settings = jnp.concatenate(
        [
            jnp.pad(window_lengths.astype(jnp.float32), (0, half - count)),
            jnp.pad(exclusion.astype(jnp.float32), (0, half - count)),
        ]
    ).reshape(1, LANES)
    spare = jnp.zeros((rows - piece_rows - 3, LANES), jnp.float32)
    return jnp.concatenate([values, slots, settings, spare], axis=0)


def gather_pieces(piece, count_tile, count_len):
    held = piece[None]
    mask = 1
    while mask < count_tile:
        if mask == 2:
            pairs = [
                (a * count_tile + b, (a ^ 1) * count_tile + (b ^ mask))
                for a in range(count_len)
                for b in range(count_tile)
            ]
            other = lax.ppermute(held, ("len", "tile"), pairs)
        else:
            other = lax.ppermute(held, "tile", [(b, b ^ mask) for b in range(count_tile)])
        mask *= 2
        if mask == count_tile:
            return held, other
        held = jnp.concatenate([held, other], axis=0)


def flat_shift(values, amount):
    rows = values.shape[0]
    whole, part = divmod(amount, LANES)
    if whole:
        values = pltpu.roll(values, (rows - whole) % rows, 0)
    if part:
        rolled = pltpu.roll(values, LANES - part, 1)
        following = pltpu.roll(rolled, rows - 1, 0)
        lane = lax.broadcasted_iota(jnp.int32, values.shape, 1)
        values = jnp.where(lane < LANES - part, rolled, following)
    return values


def kernel(
    count_tile,
    count_len,
    count_own,
    piece_length,
    first_ref,
    second_ref,
    out_ref,
    slots_ref,
    flat_ref,
    sum_ref,
    square_ref,
    shifted_ref,
    turned_ref,
    left_ref,
    right_ref,
    best_ref,
    number_ref,
    item_ref,
):
    me = lax.axis_index("tile")
    side = lax.rem(lax.axis_index("len"), 2)
    count = 2 * count_own
    half_slots = count_tile // 2
    piece_rows = -(-piece_length // LANES)
    series_rows = flat_ref.shape[0]
    blocks = TILE_SIDE // LANES
    lane_row = lax.broadcasted_iota(jnp.int32, (1, LANES), 1)

    slots_ref[:half_slots] = first_ref[...]
    slots_ref[half_slots:] = second_ref[...]

    for index in range(count):
        from_own = (index // count_own) == side
        slot = jnp.where(from_own, 0, 2)
        row = slots_ref[slot, pl.ds(piece_rows + 2, 1), :]
        for kind in range(2):
            spot = index % count_own + kind * (LANES // 2)
            number_ref[kind, index] = jnp.sum(jnp.where(lane_row == spot, row, 0.0)).astype(jnp.int32)
    row_ids = slots_ref[:, piece_rows, :].astype(jnp.int32)
    col_ids = slots_ref[:, piece_rows + 1, :].astype(jnp.int32)
    words = -(-count_tile // WORD)
    for kind, (fixed, listed) in enumerate(((row_ids, col_ids), (col_ids, row_ids))):
        for word in range(words):
            spot = listed - word * WORD
            chosen = (fixed == me) & (spot >= 0) & (spot < WORD)
            bit = jnp.left_shift(1, jnp.where(chosen, spot, 0)).astype(jnp.float32)
            number_ref[2 + kind, word] = jnp.sum(jnp.where(chosen, bit, 0.0)).astype(jnp.int32)

    def list_items(kind, start):
        def step(block, carry):
            filled, seen = carry
            present = lax.rem(lax.shift_right_logical(number_ref[2 + kind, block // WORD], lax.rem(block, WORD)), 2)
            odd = lax.rem(seen + side, 2)
            for pair in range(count // 2):
                item_ref[filled] = ((kind * count + 2 * pair + odd) * count_tile) + block
                filled = filled + present
            return filled, seen + present

        return lax.fori_loop(0, count_tile, step, start)

    filled, _ = list_items(1, list_items(0, (jnp.int32(0), jnp.int32(0))))

    flat_ref[...] = jnp.zeros_like(flat_ref)
    lane = lax.broadcasted_iota(jnp.int32, (piece_rows, LANES), 1)
    for index in range(count_tile):
        piece = slots_ref[lax.bitwise_xor(me, index), :piece_rows, :]
        row, offset = divmod(index * piece_length, LANES)
        if offset:
            piece = pltpu.roll(piece, offset, 1)
            flat_ref[row + 1 : row + 1 + piece_rows] += jnp.where(lane < offset, piece, 0.0)
            piece = jnp.where(lane < offset, 0.0, piece)
        flat_ref[row : row + piece_rows] += piece

    for index in range(count):
        sum_ref[index] = jnp.zeros((series_rows, LANES), jnp.float32)
        square_ref[index] = jnp.zeros((series_rows, LANES), jnp.float32)
    level_sum = flat_ref[...]
    level_square = jnp.zeros_like(level_sum)
    size = 1
    while True:
        for index in range(count):
            length = number_ref[0, index]

            @pl.when(lax.bitwise_and(length, size) != 0)
            def _(index=index, length=length, size=size, level_sum=level_sum, level_square=level_square):
                tail = jnp.full((1, 1), lax.bitwise_and(length, size - 1), jnp.int32).astype(jnp.float32)
                tail_sum = flat_shift(sum_ref[index], size)
                tail_square = flat_shift(square_ref[index], size)
                apart = tail_sum * (1.0 / jnp.maximum(tail, 1.0)) - level_sum * (1.0 / size)
                weight = tail * size / (tail + size)
                sum_ref[index] = level_sum + tail_sum
                square_ref[index] = level_square + tail_square + apart * apart * weight

        if size >= MAX_LEN:
            break
        next_sum = flat_shift(level_sum, size)
        next_square = flat_shift(level_square, size)
        apart = (next_sum - level_sum) * (1.0 / size)
        level_sum = level_sum + next_sum
        level_square = level_square + next_square + apart * apart * (size / 2)
        size *= 2
    for index in range(count):
        length = jnp.full((1, 1), number_ref[0, index], jnp.int32).astype(jnp.float32)
        sum_ref[index] = sum_ref[index] / length
        square_ref[index] = 1.0 / jnp.sqrt(square_ref[index] / length + VAR_EPS)

    square_row = lax.broadcasted_iota(jnp.int32, (LANES, LANES), 0)
    square_lane = lax.broadcasted_iota(jnp.int32, (LANES, LANES), 1)
    inside = square_lane <= square_row

    def rotated(row):
        values = jnp.broadcast_to(flat_ref[pl.ds(row, 1), :], (LANES, LANES))
        return pltpu.roll(values, 1, 1, stride=1, stride_axis=0)

    def shift_row(row, current):
        following = rotated(row + 1)
        shifted_ref[row] = jnp.where(inside, current, following)
        return following

    lax.fori_loop(0, series_rows - 1, shift_row, rotated(0))

    best_ref[...] = jnp.full_like(best_ref, LOWEST)
    for spot in range(blocks + MAX_LEN // LANES - 1):
        turned_ref[spot] = shifted_ref[me * blocks + spot].T
    for index in range(count):
        length = number_ref[0, index]
        chunks = (length + CHUNK - 1) // CHUNK
        for block in range(blocks):
            row = me * blocks + block
            centre = jnp.broadcast_to(sum_ref[index, pl.ds(row, 1), :], (LANES, LANES)).T
            inverse = jnp.broadcast_to(square_ref[index, pl.ds(row, 1), :], (LANES, LANES)).T
            for chunk in range(MAX_LEN // CHUNK):

                @pl.when(chunk < chunks)
                def _(index=index, block=block, chunk=chunk, centre=centre, inverse=inverse, length=length):
                    for part in range(CHUNK // LANES):
                        spot = chunk * (CHUNK // LANES) + part
                        values = (turned_ref[block + spot] - centre) * inverse
                        values = jnp.where(LANES - 1 - square_lane < length - spot * LANES, values, 0.0)
                        left_ref[
                            index, block * LANES : (block + 1) * LANES, spot * LANES : (spot + 1) * LANES
                        ] = values.astype(jnp.bfloat16)

    def one_item(position, carry):
        item = item_ref[position]
        other = lax.rem(item, count_tile)
        target = item // count_tile
        kind = target // count
        index = lax.rem(target, count)
        length = number_ref[0, index]
        barrier = number_ref[1, index]
        chunks = (length + CHUNK - 1) // CHUNK
        ahead = jnp.where(kind == 0, 1, -1)
        gap = ahead * (other - me) * TILE_SIDE
        near = gap - (TILE_SIDE - 1) <= barrier

        for steps in range(1, MAX_LEN // CHUNK + 1):
            for masked in (False, True):

                @pl.when((chunks == steps) & (near == masked))
                def _(steps=steps, masked=masked):
                    for block in range(blocks):
                        row = other * blocks + block
                        centre = sum_ref[index, pl.ds(row, 1), :]
                        inverse = square_ref[index, pl.ds(row, 1), :]
                        for spot in range(steps * (CHUNK // LANES)):
                            values = (shifted_ref[row + spot] - centre) * inverse
                            right_ref[
                                spot * LANES : (spot + 1) * LANES, block * LANES : (block + 1) * LANES
                            ] = values.astype(jnp.bfloat16)
                    depth = steps * CHUNK
                    product = jnp.dot(
                        left_ref[index, :, :depth], right_ref[:depth, :], preferred_element_type=jnp.float32
                    )
                    if masked:
                        own_ids = lax.broadcasted_iota(jnp.int32, product.shape, 0)
                        other_ids = lax.broadcasted_iota(jnp.int32, product.shape, 1)
                        product = jnp.where(gap + ahead * (other_ids - own_ids) > barrier, product, LOWEST)
                    best = best_ref[target]
                    for block in range(blocks):
                        best = jnp.maximum(best, product[:, block * LANES : (block + 1) * LANES])
                    best_ref[target] = best

        return carry

    lax.fori_loop(0, filled, one_item, jnp.int32(0))

    for target in range(2 * count):
        length = jnp.full((1, 1), number_ref[0, target % count], jnp.int32).astype(jnp.float32)
        for block in range(blocks):
            best = best_ref[target, block * LANES : (block + 1) * LANES, :].T
            best = jnp.max(best, axis=0, keepdims=True)
            out_ref[target : target + 1, block * LANES : (block + 1) * LANES] = jnp.minimum(
                1.0 - best / length, EMPTY_VALUE
            )


def local_profiles(first, second, count_tile, count_len, count_own, piece_length):
    count = 2 * count_own
    series_rows = round_up(count_tile * piece_length, 8 * LANES) // LANES + 8
    slots = (count_tile,) + first.shape[1:]
    return pl.pallas_call(
        functools.partial(kernel, count_tile, count_len, count_own, piece_length),
        out_shape=jax.ShapeDtypeStruct((2 * count, TILE_SIDE), jnp.float32),
        in_specs=[pl.BlockSpec(memory_space=pltpu.VMEM)] * 2,
        out_specs=pl.BlockSpec(memory_space=pltpu.VMEM),
        scratch_shapes=[
            pltpu.VMEM(slots, jnp.float32),
            pltpu.VMEM((series_rows, LANES), jnp.float32),
            pltpu.VMEM((count, series_rows, LANES), jnp.float32),
            pltpu.VMEM((count, series_rows, LANES), jnp.float32),
            pltpu.VMEM((series_rows, LANES, LANES), jnp.float32),
            pltpu.VMEM(((TILE_SIDE + MAX_LEN) // LANES - 1, LANES, LANES), jnp.float32),
            pltpu.VMEM((count, TILE_SIDE, MAX_LEN), jnp.bfloat16),
            pltpu.VMEM((MAX_LEN, TILE_SIDE), jnp.bfloat16),
            pltpu.VMEM((2 * count, TILE_SIDE, LANES), jnp.float32),
            pltpu.SMEM((4, max(count, -(-count_tile // WORD))), jnp.int32),
            pltpu.SMEM((2 * count_tile * count + count,), jnp.int32),
        ],
        compiler_params=pltpu.CompilerParams(vmem_limit_bytes=56 * 2**20),
        name="profiles",
    )(first, second)


def shards(series, window_lengths, exclusion, tile_list):
    count_tile, count_len = lax.axis_size("tile"), lax.axis_size("len")
    count_own = window_lengths.shape[0]
    piece = packed_piece(series, window_lengths, exclusion, tile_list)
    first, second = gather_pieces(piece, count_tile, count_len)
    local = local_profiles(first, second, count_tile, count_len, count_own, series.shape[0])
    merged = jnp.minimum(local, lax.ppermute(local, "len", [(a, a ^ 1) for a in range(count_len)]))
    merged = merged.reshape(2, 2 * count_own, TILE_SIDE)
    if count_len > 2:
        groups = [list(range(a, count_len, 2)) for a in range(2)]
        merged = lax.all_gather(merged, "len", axis=1, tiled=True, axis_index_groups=groups)
    return merged[0], merged[1]


def solution(mesh):
    return jax.shard_map(
        shards,
        mesh=mesh,
        in_specs=(P("tile"), P("len"), P("len"), P("tile", None)),
        out_specs=(P(None, "tile"), P(None, "tile")),
        check_vma=False,
    )
```

```python
import functools

import jax
import jax.numpy as jnp
from jax import lax
from jax.experimental import pallas as pl
from jax.experimental.pallas import tpu as pltpu
from jax.sharding import PartitionSpec as P

MAX_LEN = 1024
TILE_SIDE = 512
EMPTY_VALUE = 2.0
VAR_EPS = 1e-05
LANES = 128
CHUNK = 256
LOWEST = -3.0e38
WORD = 16
MAX_EXCLUSION = 256


def round_up(value, multiple):
    return (value + multiple - 1) // multiple * multiple


def packed_piece(series, window_lengths, exclusion, tile_list):
    piece_rows = -(-series.shape[0] // LANES)
    rows = round_up(piece_rows + 3, 8)
    values = jnp.pad(series, (0, piece_rows * LANES - series.shape[0])).reshape(piece_rows, LANES)
    slots = tile_list.astype(jnp.float32).T
    slots = jnp.pad(slots, ((0, 0), (0, LANES - slots.shape[1])), constant_values=-1.0)
    half = LANES // 2
    count = window_lengths.shape[0]
    settings = jnp.concatenate(
        [
            jnp.pad(window_lengths.astype(jnp.float32), (0, half - count)),
            jnp.pad(exclusion.astype(jnp.float32), (0, half - count)),
        ]
    ).reshape(1, LANES)
    spare = jnp.zeros((rows - piece_rows - 3, LANES), jnp.float32)
    return jnp.concatenate([values, slots, settings, spare], axis=0)


def gather_pieces(piece, count_tile, count_len):
    held = piece[None]
    mask = 1
    while mask < count_tile:
        if mask == 2:
            pairs = [
                (a * count_tile + b, (a ^ 1) * count_tile + (b ^ mask))
                for a in range(count_len)
                for b in range(count_tile)
            ]
            other = lax.ppermute(held, ("len", "tile"), pairs)
        else:
            other = lax.ppermute(held, "tile", [(b, b ^ mask) for b in range(count_tile)])
        mask *= 2
        if mask == count_tile:
            return held, other
        held = jnp.concatenate([held, other], axis=0)


def flat_shift(values, amount):
    rows = values.shape[0]
    whole, part = divmod(amount, LANES)
    if whole:
        values = pltpu.roll(values, (rows - whole) % rows, 0)
    if part:
        rolled = pltpu.roll(values, LANES - part, 1)
        following = pltpu.roll(rolled, rows - 1, 0)
        lane = lax.broadcasted_iota(jnp.int32, values.shape, 1)
        values = jnp.where(lane < LANES - part, rolled, following)
    return values


def kernel(
    count_tile,
    count_own,
    piece_length,
    first_ref,
    second_ref,
    out_ref,
    slots_ref,
    flat_ref,
    sum_ref,
    square_ref,
    shifted_ref,
    turned_ref,
    left_ref,
    even_ref,
    odd_ref,
    best_ref,
    number_ref,
    tile_ref,
):
    me = lax.axis_index("tile")
    side = lax.rem(lax.axis_index("len"), 2)
    count = 2 * count_own
    half_slots = count_tile // 2
    piece_rows = -(-piece_length // LANES)
    series_rows = sum_ref.shape[1]
    blocks = TILE_SIDE // LANES
    lane_row = lax.broadcasted_iota(jnp.int32, (1, LANES), 1)
    square_row = lax.broadcasted_iota(jnp.int32, (LANES, LANES), 0)
    square_lane = lax.broadcasted_iota(jnp.int32, (LANES, LANES), 1)

    with jax.named_scope("numbers"):
        slots_ref[:half_slots] = first_ref[...]
        slots_ref[half_slots:] = second_ref[...]

        for index in range(count):
            from_own = (index // count_own) == side
            slot = jnp.where(from_own, 0, 2)
            row = slots_ref[slot, pl.ds(piece_rows + 2, 1), :]
            for kind in range(2):
                spot = index % count_own + kind * (LANES // 2)
                number_ref[kind, index] = jnp.sum(jnp.where(lane_row == spot, row, 0.0)).astype(jnp.int32)
        row_ids = slots_ref[:, piece_rows, :].astype(jnp.int32)
        col_ids = slots_ref[:, piece_rows + 1, :].astype(jnp.int32)
        near = (col_ids - row_ids) * TILE_SIDE - (TILE_SIDE - 1) <= MAX_EXCLUSION

        def word_of(chosen, spot):
            chosen = chosen & (spot >= 0) & (spot < WORD)
            bit = jnp.left_shift(1, jnp.where(chosen, spot, 0)).astype(jnp.float32)
            return jnp.sum(jnp.where(chosen, bit, 0.0)).astype(jnp.int32)

        words = [
            [word_of((fixed == me) & ~near, listed - word * WORD) for word in range(-(-count_tile // WORD))]
            for fixed, listed in ((row_ids, col_ids), (col_ids, row_ids))
        ]
        near_words = [word_of((fixed == me) & near, col_ids - row_ids) for fixed in (row_ids, col_ids)]

    with jax.named_scope("list"):
        far_count = jnp.int32(0)
        for kind in range(2):
            for block in range(count_tile):
                tile_ref[0, far_count] = kind * count_tile + block
                word = words[kind][block // WORD]
                far_count = far_count + lax.bitwise_and(lax.shift_right_logical(word, block % WORD), 1)
        near_count = jnp.int32(0)
        for kind in range(2):
            for gap in range(WORD):
                if gap * TILE_SIDE - (TILE_SIDE - 1) <= MAX_EXCLUSION:
                    tile_ref[1, near_count] = kind * count_tile + me + (gap if kind == 0 else -gap)
                    near_count = near_count + lax.bitwise_and(lax.shift_right_logical(near_words[kind], gap), 1)

    with jax.named_scope("flat"):
        flat_ref[...] = jnp.zeros_like(flat_ref)
        lane = lax.broadcasted_iota(jnp.int32, (piece_rows, LANES), 1)
        for index in range(count_tile):
            piece = slots_ref[lax.bitwise_xor(me, index), :piece_rows, :]
            row, offset = divmod(index * piece_length, LANES)
            if offset:
                piece = pltpu.roll(piece, offset, 1)
                flat_ref[row + 1 : row + 1 + piece_rows] += jnp.where(lane < offset, piece, 0.0)
                piece = jnp.where(lane < offset, 0.0, piece)
            flat_ref[row : row + piece_rows] += piece

    inside = square_lane <= square_row

    def rotated(row):
        values = jnp.broadcast_to(flat_ref[row : row + 1, :], (LANES, LANES))
        return pltpu.roll(values, 1, 1, stride=1, stride_axis=0)

    def shift_rows(first, last):
        if first >= last:
            return
        current = rotated(first)
        for row in range(first, last):
            following = rotated(row + 1)
            shifted_ref[row] = jnp.where(inside, current, following)
            current = following

    with jax.named_scope("stats"):
        for index in range(count):
            sum_ref[index] = jnp.zeros((series_rows, LANES), jnp.float32)
            square_ref[index] = jnp.zeros((series_rows, LANES), jnp.float32)
        level_sum = flat_ref[:series_rows]
        level_square = jnp.zeros_like(level_sum)
        size = 1
        done = 0
        share = -(-(series_rows - 1) // (MAX_LEN.bit_length() - 1))
        while True:
            for index in range(count):
                length = number_ref[0, index]

                @pl.when(lax.bitwise_and(length, size) != 0)
                def _(index=index, length=length, size=size, level_sum=level_sum, level_square=level_square):
                    tail = jnp.full((1, 1), lax.bitwise_and(length, size - 1), jnp.int32).astype(jnp.float32)
                    tail_sum = flat_shift(sum_ref[index], size)
                    tail_square = flat_shift(square_ref[index], size)
                    apart = tail_sum * (1.0 / jnp.maximum(tail, 1.0)) - level_sum * (1.0 / size)
                    weight = tail * size / (tail + size)
                    sum_ref[index] = level_sum + tail_sum
                    square_ref[index] = level_square + tail_square + apart * apart * weight

            if size >= MAX_LEN:
                break
            next_sum = flat_shift(level_sum, size)
            next_square = flat_shift(level_square, size)
            apart = (next_sum - level_sum) * (1.0 / size)
            level_sum = level_sum + next_sum
            level_square = level_square + next_square + apart * apart * (size / 2)
            size *= 2
            shift_rows(done, min(done + share, series_rows - 1))
            done += share
        for index in range(count):
            length = jnp.full((1, 1), number_ref[0, index], jnp.int32).astype(jnp.float32)
            sum_ref[index] = sum_ref[index] / length
            square_ref[index] = 1.0 / jnp.sqrt(square_ref[index] / length + VAR_EPS)
        for spot in range(blocks + MAX_LEN // LANES - 1):
            turned_ref[spot] = shifted_ref[me * blocks + spot].T

    def per_length(index, carry):
        length = number_ref[0, index]
        barrier = number_ref[1, index]
        chunks = (length + CHUNK - 1) // CHUNK
        near_start = lax.rem(index + side, 2)
        far_start = lax.rem(index + side + near_count, 2)
        far_last = far_start + 2 * ((far_count - far_start + 1) // 2 - 1)
        best_ref[index] = jnp.full_like(best_ref[index], LOWEST)
        best_ref[count + index] = jnp.full_like(best_ref[index], LOWEST)

        for steps in range(1, MAX_LEN // CHUNK + 1):
            depth = steps * CHUNK

            def build(operand_ref, tile, depth=depth):
                other = lax.rem(tile, count_tile)
                for block in range(blocks):
                    row = other * blocks + block
                    centre = sum_ref[index, pl.ds(row, 1), :]
                    inverse = square_ref[index, pl.ds(row, 1), :]
                    for spot in range(depth // LANES):
                        values = (shifted_ref[row + spot] - centre) * inverse
                        operand_ref[
                            spot * LANES : (spot + 1) * LANES, block * LANES : (block + 1) * LANES
                        ] = values.astype(jnp.bfloat16)

            def multiply(operand_ref, tile, masked, depth=depth):
                kind = tile // count_tile
                product = jnp.dot(left_ref[:, :depth], operand_ref[:depth, :], preferred_element_type=jnp.float32)
                if masked:
                    ahead = 1 - 2 * kind
                    gap = ahead * (lax.rem(tile, count_tile) - me) * TILE_SIDE
                    own_ids = lax.broadcasted_iota(jnp.int32, product.shape, 0)
                    other_ids = lax.broadcasted_iota(jnp.int32, product.shape, 1)
                    product = jnp.where(gap + ahead * (other_ids - own_ids) > barrier, product, LOWEST)
                best = best_ref[kind * count + index]
                for block in range(blocks):
                    best = jnp.maximum(best, product[:, block * LANES : (block + 1) * LANES])
                best_ref[kind * count + index] = best

            @pl.when(chunks == steps)
            def _(depth=depth, build=build, multiply=multiply):
                with jax.named_scope("own"):
                    for block in range(blocks):
                        row = me * blocks + block
                        centre = jnp.broadcast_to(sum_ref[index, pl.ds(row, 1), :], (LANES, LANES)).T
                        inverse = jnp.broadcast_to(square_ref[index, pl.ds(row, 1), :], (LANES, LANES)).T
                        for spot in range(depth // LANES):
                            values = (turned_ref[block + spot] - centre) * inverse
                            if spot >= (depth - CHUNK) // LANES:
                                values = jnp.where(LANES - 1 - square_lane < length - spot * LANES, values, 0.0)
                            left_ref[
                                block * LANES : (block + 1) * LANES, spot * LANES : (spot + 1) * LANES
                            ] = values.astype(jnp.bfloat16)
                    build(even_ref, tile_ref[0, jnp.maximum(far_last, 0)])

                def near_tile(position, carry):
                    with jax.named_scope("near"):
                        tile = tile_ref[1, near_start + 2 * position]
                        build(odd_ref, tile)
                        multiply(odd_ref, tile, True)
                    return carry

                lax.fori_loop(0, (near_count - near_start + 1) // 2, near_tile, jnp.int32(0))

                def far_pair(position, carry):
                    spot = far_last - 4 * position
                    tiles = [tile_ref[0, jnp.maximum(spot - 2 * step, 0)] for step in range(3)]
                    with jax.named_scope("far"):
                        multiply(even_ref, tiles[0], False)
                        build(odd_ref, tiles[1])

                    @pl.when(spot - 2 >= far_start)
                    def _():
                        with jax.named_scope("far"):
                            multiply(odd_ref, tiles[1], False)
                            build(even_ref, tiles[2])

                    return carry

                lax.fori_loop(0, ((far_count - far_start + 1) // 2 + 1) // 2, far_pair, jnp.int32(0))

        return carry

    lax.fori_loop(0, count, per_length, jnp.int32(0))

    with jax.named_scope("final"):
        for target in range(2 * count):
            length = jnp.full((1, 1), number_ref[0, target % count], jnp.int32).astype(jnp.float32)
            for block in range(blocks):
                best = best_ref[target, block * LANES : (block + 1) * LANES, :].T
                best = jnp.max(best, axis=0, keepdims=True)
                out_ref[target : target + 1, block * LANES : (block + 1) * LANES] = jnp.minimum(
                    1.0 - best / length, EMPTY_VALUE
                )


def local_profiles(first, second, count_tile, count_own, piece_length):
    count = 2 * count_own
    series_rows = round_up(count_tile * piece_length, 8 * LANES) // LANES
    vectors = [
        ((count_tile,) + first.shape[1:], jnp.float32),
        ((round_up(series_rows + first.shape[1], 8), LANES), jnp.float32),
        ((count, series_rows, LANES), jnp.float32),
        ((count, series_rows, LANES), jnp.float32),
        ((series_rows, LANES, LANES), jnp.float32),
        (((TILE_SIDE + MAX_LEN) // LANES - 1, LANES, LANES), jnp.float32),
        ((TILE_SIDE, MAX_LEN), jnp.bfloat16),
        ((MAX_LEN, TILE_SIDE), jnp.bfloat16),
        ((MAX_LEN, TILE_SIDE), jnp.bfloat16),
        ((2 * count, TILE_SIDE, LANES), jnp.float32),
    ]
    used = sum(jnp.dtype(kind).itemsize * functools.reduce(lambda a, b: a * b, shape) for shape, kind in vectors)
    return pl.pallas_call(
        functools.partial(kernel, count_tile, count_own, piece_length),
        out_shape=jax.ShapeDtypeStruct((2 * count, TILE_SIDE), jnp.float32),
        in_specs=[pl.BlockSpec(memory_space=pltpu.VMEM)] * 2,
        out_specs=pl.BlockSpec(memory_space=pltpu.VMEM),
        scratch_shapes=[pltpu.VMEM(shape, kind) for shape, kind in vectors]
        + [
            pltpu.SMEM((2, max(count, count_tile)), jnp.int32),
            pltpu.SMEM((2, 2 * count_tile + 2), jnp.int32),
        ],
        compiler_params=pltpu.CompilerParams(vmem_limit_bytes=used + 6 * 2**20),
        name="profiles",
    )(first, second)


def shards(series, window_lengths, exclusion, tile_list):
    count_tile, count_len = lax.axis_size("tile"), lax.axis_size("len")
    count_own = window_lengths.shape[0]
    piece = packed_piece(series, window_lengths, exclusion, tile_list)
    first, second = gather_pieces(piece, count_tile, count_len)
    local = local_profiles(first, second, count_tile, count_own, series.shape[0])
    merged = jnp.minimum(local, lax.ppermute(local, "len", [(a, a ^ 1) for a in range(count_len)]))
    merged = merged.reshape(2, 2 * count_own, TILE_SIDE)
    if count_len > 2:
        groups = [list(range(a, count_len, 2)) for a in range(2)]
        merged = lax.all_gather(merged, "len", axis=1, tiled=True, axis_index_groups=groups)
    return merged[0], merged[1]


def solution(mesh):
    return jax.shard_map(
        shards,
        mesh=mesh,
        in_specs=(P("tile"), P("len"), P("len"), P("tile", None)),
        out_specs=(P(None, "tile"), P(None, "tile")),
        check_vma=False,
    )
```

```python
import functools
import math

import jax
import jax.numpy as jnp
from jax import lax
from jax.experimental import pallas as pl
from jax.experimental.pallas import tpu as pltpu
from jax.sharding import PartitionSpec as P

MAX_LEN = 1024
TILE_SIDE = 512
EMPTY_VALUE = 2.0
VAR_EPS = 1e-05
MAX_EXCLUSION = 256
LANES = 128
CHUNK = 256
LOWEST = -3.0e38
WORD = 16


def round_up(value, multiple):
    return (value + multiple - 1) // multiple * multiple


def pack_kernel(length_ref, exclusion_ref, tile_ref, series_ref, out_ref):
    piece_rows = -(-series_ref.shape[0] // LANES)
    lane = lax.broadcasted_iota(jnp.int32, (1, LANES), 1)
    out_ref[...] = jnp.zeros_like(out_ref)
    for row in range(piece_rows):
        held = min(LANES, series_ref.shape[0] - row * LANES)
        out_ref[row : row + 1, :held] = series_ref[row * LANES : row * LANES + held].reshape(1, held)
    for side in range(2):
        values = jnp.full((1, LANES), -1, jnp.int32)
        for slot in range(tile_ref.shape[0]):
            values = jnp.where(lane == slot, tile_ref[slot, side], values)
        out_ref[piece_rows + side : piece_rows + side + 1, :] = values.astype(jnp.float32)
    values = jnp.zeros((1, LANES), jnp.int32)
    for index in range(length_ref.shape[0]):
        values = jnp.where(lane == index, length_ref[index], values)
        values = jnp.where(lane == LANES // 2 + index, exclusion_ref[index], values)
    out_ref[piece_rows + 2 : piece_rows + 3, :] = values.astype(jnp.float32)


def packed_piece(series, window_lengths, exclusion, tile_list):
    rows = round_up(-(-series.shape[0] // LANES) + 3, 8)
    scalars = pl.BlockSpec(memory_space=pltpu.SMEM)
    return pl.pallas_call(
        pack_kernel,
        out_shape=jax.ShapeDtypeStruct((rows, LANES), jnp.float32),
        in_specs=[scalars, scalars, scalars, pl.BlockSpec(memory_space=pltpu.VMEM)],
        out_specs=pl.BlockSpec(memory_space=pltpu.VMEM),
        compiler_params=pltpu.CompilerParams(vmem_limit_bytes=2**20),
        name="pack",
    )(window_lengths, exclusion, tile_list, series)


def gather_pieces(piece, count_tile):
    held = piece[None]
    mask = 1
    while True:
        other = lax.ppermute(held, "tile", [(b, b ^ mask) for b in range(count_tile)])
        mask *= 2
        if mask == count_tile:
            return held, other
        held = jnp.concatenate([held, other], axis=0)


def flat_shift(values, amount):
    rows = values.shape[0]
    whole, part = divmod(amount, LANES)
    if whole:
        values = pltpu.roll(values, (rows - whole) % rows, 0)
    if part:
        rolled = pltpu.roll(values, LANES - part, 1)
        following = pltpu.roll(rolled, rows - 1, 0)
        lane = lax.broadcasted_iota(jnp.int32, values.shape, 1)
        values = jnp.where(lane < LANES - part, rolled, following)
    return values


def kernel(
    count_tile,
    count,
    piece_length,
    first_ref,
    second_ref,
    out_ref,
    slots_ref,
    flat_ref,
    centre_ref,
    inverse_ref,
    shifted_ref,
    turned_ref,
    left_ref,
    even_ref,
    odd_ref,
    best_ref,
    number_ref,
    tile_ref,
):
    me = lax.axis_index("tile")
    half_slots = count_tile // 2
    piece_rows = -(-piece_length // LANES)
    series_rows = centre_ref.shape[1]
    blocks = TILE_SIDE // LANES
    lane_row = lax.broadcasted_iota(jnp.int32, (1, LANES), 1)
    square_row = lax.broadcasted_iota(jnp.int32, (LANES, LANES), 0)
    square_lane = lax.broadcasted_iota(jnp.int32, (LANES, LANES), 1)

    with jax.named_scope("numbers"):
        slots_ref[:half_slots] = first_ref[...]
        slots_ref[half_slots:] = second_ref[...]

        settings = first_ref[0, piece_rows + 2 : piece_rows + 3, :]
        for index in range(count):
            for kind in range(2):
                spot = index + kind * (LANES // 2)
                number_ref[kind, index] = jnp.sum(jnp.where(lane_row == spot, settings, 0.0)).astype(jnp.int32)
        row_ids = slots_ref[:, piece_rows, :].astype(jnp.int32)
        col_ids = slots_ref[:, piece_rows + 1, :].astype(jnp.int32)
        near = (col_ids - row_ids) * TILE_SIDE - (TILE_SIDE - 1) <= MAX_EXCLUSION
        reach = (MAX_EXCLUSION + TILE_SIDE - 1) // TILE_SIDE

        def word_of(chosen, spot):
            chosen = chosen & (spot >= 0) & (spot < WORD)
            bit = jnp.left_shift(1, jnp.where(chosen, spot, 0)).astype(jnp.float32)
            return jnp.sum(jnp.where(chosen, bit, 0.0)).astype(jnp.int32)

        words = [
            [word_of((fixed == me) & ~near, listed - word * WORD) for word in range(-(-count_tile // WORD))]
            for fixed, listed in ((row_ids, col_ids), (col_ids, row_ids))
        ]
        around = jnp.where(row_ids == me, col_ids, row_ids) - me + reach
        near_word = word_of(((row_ids == me) | (col_ids == me)) & near, around)

    with jax.named_scope("list"):
        far_count = jnp.int32(0)
        for kind in range(2):
            for block in range(count_tile):
                tile_ref[0, far_count] = kind * count_tile + block
                word = words[kind][block // WORD]
                far_count = far_count + lax.bitwise_and(lax.shift_right_logical(word, block % WORD), 1)
        near_count = jnp.int32(0)
        for spot in range(2 * reach + 1):
            tile_ref[1, near_count] = me + spot - reach
            near_count = near_count + lax.bitwise_and(lax.shift_right_logical(near_word, spot), 1)

    with jax.named_scope("flat"):
        flat_ref[...] = jnp.zeros_like(flat_ref)
        lane = lax.broadcasted_iota(jnp.int32, (piece_rows, LANES), 1)
        for index in range(count_tile):
            piece = slots_ref[lax.bitwise_xor(me, index), :piece_rows, :]
            row, offset = divmod(index * piece_length, LANES)
            if offset:
                piece = pltpu.roll(piece, offset, 1)
                flat_ref[row + 1 : row + 1 + piece_rows] += jnp.where(lane < offset, piece, 0.0)
                piece = jnp.where(lane < offset, 0.0, piece)
            flat_ref[row : row + piece_rows] += piece

    inside = square_lane <= square_row

    def rotated(row):
        values = jnp.broadcast_to(flat_ref[row : row + 1, :], (LANES, LANES))
        return pltpu.roll(values, 1, 1, stride=1, stride_axis=0)

    def shift_rows(first, last):
        if first >= last:
            return
        current = rotated(first)
        for row in range(first, last):
            following = rotated(row + 1)
            shifted_ref[row] = jnp.where(inside, current, following)
            current = following

    with jax.named_scope("stats"):
        level_sum = flat_ref[:series_rows]
        level_square = jnp.zeros_like(level_sum)
        sums = [level_square] * count
        squares = [level_square] * count
        size = 1
        done = 0
        share = -(-(series_rows - 1) // MAX_LEN.bit_length())
        while True:
            for index in range(count):
                length = number_ref[0, index]
                taken = lax.bitwise_and(length, size) != 0
                tail = jnp.full((1, 1), lax.bitwise_and(length, size - 1), jnp.int32).astype(jnp.float32)
                tail_sum = flat_shift(sums[index], size)
                tail_square = flat_shift(squares[index], size)
                apart = tail_sum * (1.0 / jnp.maximum(tail, 1.0)) - level_sum * (1.0 / size)
                weight = tail * size / (tail + size)
                squares[index] = jnp.where(
                    taken, level_square + tail_square + apart * apart * weight, squares[index]
                )
                sums[index] = jnp.where(taken, level_sum + tail_sum, sums[index])
            shift_rows(done, min(done + share, series_rows - 1))
            done += share
            if size >= MAX_LEN:
                break
            next_sum = flat_shift(level_sum, size)
            next_square = flat_shift(level_square, size)
            apart = (next_sum - level_sum) * (1.0 / size)
            level_sum = level_sum + next_sum
            level_square = level_square + next_square + apart * apart * (size / 2)
            size *= 2
        for index in range(count):
            length = jnp.full((1, 1), number_ref[0, index], jnp.int32).astype(jnp.float32)
            centre_ref[index] = sums[index] / length
            inverse_ref[index] = 1.0 / jnp.sqrt(squares[index] / length + VAR_EPS)
        for spot in range(blocks + MAX_LEN // LANES - 1):
            turned_ref[spot] = shifted_ref[me * blocks + spot].T

    def per_length(index, carry):
        length = number_ref[0, index]
        barrier = number_ref[1, index]
        chunks = (length + CHUNK - 1) // CHUNK
        best_ref[index] = jnp.full_like(best_ref[index], LOWEST)
        best_ref[count + index] = jnp.full_like(best_ref[index], LOWEST)

        for steps in range(1, MAX_LEN // CHUNK + 1):
            depth = steps * CHUNK

            def build(operand_ref, other, chunk):
                for block in range(blocks):
                    row = other * blocks + block
                    centre = centre_ref[index, pl.ds(row, 1), :]
                    inverse = inverse_ref[index, pl.ds(row, 1), :]
                    for spot in range(chunk * CHUNK // LANES, (chunk + 1) * CHUNK // LANES):
                        values = (shifted_ref[row + spot] - centre) * inverse
                        operand_ref[
                            spot * LANES : (spot + 1) * LANES, block * LANES : (block + 1) * LANES
                        ] = values.astype(jnp.bfloat16)

            def partial(operand_ref, chunk):
                part = slice(chunk * CHUNK, (chunk + 1) * CHUNK)
                return jnp.dot(left_ref[:, part], operand_ref[part, :], preferred_element_type=jnp.float32)

            def improve(target, product):
                best = best_ref[target]
                for block in range(blocks):
                    best = jnp.maximum(best, product[:, block * LANES : (block + 1) * LANES])
                best_ref[target] = best

            @pl.when(chunks == steps)
            def _(steps=steps, depth=depth, build=build, partial=partial, improve=improve):
                def far(spot):
                    return tile_ref[0, jnp.clip(spot, 0, jnp.maximum(far_count - 1, 0))]

                with jax.named_scope(f"own{depth}"):
                    for block in range(blocks):
                        row = me * blocks + block
                        centre = jnp.broadcast_to(centre_ref[index, pl.ds(row, 1), :], (LANES, LANES)).T
                        inverse = jnp.broadcast_to(inverse_ref[index, pl.ds(row, 1), :], (LANES, LANES)).T
                        for spot in range(depth // LANES):
                            values = (turned_ref[block + spot] - centre) * inverse
                            if spot >= (depth - CHUNK) // LANES:
                                values = jnp.where(LANES - 1 - square_lane < length - spot * LANES, values, 0.0)
                            left_ref[
                                block * LANES : (block + 1) * LANES, spot * LANES : (spot + 1) * LANES
                            ] = values.astype(jnp.bfloat16)
                    for chunk in range(steps):
                        build(even_ref, lax.rem(far(0), count_tile), chunk)

                def near_tile(position, carry):
                    with jax.named_scope(f"near{depth}"):
                        other = tile_ref[1, position]
                        product = None
                        for chunk in range(steps):
                            build(odd_ref, other, chunk)
                            part = partial(odd_ref, chunk)
                            product = part if product is None else product + part
                        own_ids = lax.broadcasted_iota(jnp.int32, product.shape, 0)
                        other_ids = lax.broadcasted_iota(jnp.int32, product.shape, 1)
                        ahead = other_ids - own_ids
                        gap = (other - me) * TILE_SIDE
                        improve(index, jnp.where(ahead > barrier - gap, product, LOWEST))
                        improve(count + index, jnp.where(ahead < -barrier - gap, product, LOWEST))
                    return carry

                lax.fori_loop(0, near_count, near_tile, jnp.int32(0))

                def far_tile(spot, operand_ref, following_ref):
                    with jax.named_scope(f"far{depth}"):
                        following = lax.rem(far(spot + 1), count_tile)
                        product = None
                        for chunk in range(steps):
                            part = partial(operand_ref, chunk)
                            product = part if product is None else product + part
                            build(following_ref, following, chunk)
                        improve(far(spot) // count_tile * count + index, product)

                def far_pair(position, carry):
                    far_tile(2 * position, even_ref, odd_ref)

                    @pl.when(2 * position + 1 < far_count)
                    def _():
                        far_tile(2 * position + 1, odd_ref, even_ref)

                    return carry

                lax.fori_loop(0, (far_count + 1) // 2, far_pair, jnp.int32(0))

        return carry

    lax.fori_loop(0, count, per_length, jnp.int32(0))

    with jax.named_scope("final"):
        for target in range(2 * count):
            length = jnp.full((1, 1), number_ref[0, target % count], jnp.int32).astype(jnp.float32)
            for block in range(blocks):
                best = best_ref[target, block * LANES : (block + 1) * LANES, :].T
                best = jnp.max(best, axis=0, keepdims=True)
                out_ref[target : target + 1, block * LANES : (block + 1) * LANES] = jnp.minimum(
                    1.0 - best / length, EMPTY_VALUE
                )


def local_profiles(first, second, count_tile, count, piece_length):
    series_rows = round_up(count_tile * piece_length, 8 * LANES) // LANES
    vectors = [
        ((count_tile,) + first.shape[1:], jnp.float32),
        ((round_up(series_rows + first.shape[1], 8), LANES), jnp.float32),
        ((count, series_rows, LANES), jnp.float32),
        ((count, series_rows, LANES), jnp.float32),
        ((series_rows, LANES, LANES), jnp.float32),
        (((TILE_SIDE + MAX_LEN) // LANES - 1, LANES, LANES), jnp.float32),
        ((TILE_SIDE, MAX_LEN), jnp.bfloat16),
        ((MAX_LEN, TILE_SIDE), jnp.bfloat16),
        ((MAX_LEN, TILE_SIDE), jnp.bfloat16),
        ((2 * count, TILE_SIDE, LANES), jnp.float32),
    ]
    used = sum(math.prod(shape) * jnp.dtype(kind).itemsize for shape, kind in vectors)
    return pl.pallas_call(
        functools.partial(kernel, count_tile, count, piece_length),
        out_shape=jax.ShapeDtypeStruct((2 * count, TILE_SIDE), jnp.float32),
        in_specs=[pl.BlockSpec(memory_space=pltpu.VMEM)] * 2,
        out_specs=pl.BlockSpec(memory_space=pltpu.VMEM),
        scratch_shapes=[pltpu.VMEM(shape, kind) for shape, kind in vectors]
        + [pltpu.SMEM((2, count), jnp.int32), pltpu.SMEM((2, 2 * count_tile + 1), jnp.int32)],
        compiler_params=pltpu.CompilerParams(vmem_limit_bytes=used + 8 * 2**20),
        name="profiles",
    )(first, second)


def shards(series, window_lengths, exclusion, tile_list):
    count_tile, count_len = lax.axis_size("tile"), lax.axis_size("len")
    count = window_lengths.shape[0]
    piece = packed_piece(series, window_lengths, exclusion, tile_list)
    first, second = gather_pieces(piece, count_tile)
    local = local_profiles(first, second, count_tile, count, series.shape[0])
    if count_len == 2:
        other = lax.ppermute(local, "len", [(0, 1), (1, 0)])
        swap = lax.axis_index("len") == 1
        low, high = jnp.where(swap, other, local), jnp.where(swap, local, other)
        return (
            jnp.concatenate([low[:count], high[:count]], axis=0),
            jnp.concatenate([low[count:], high[count:]], axis=0),
        )
    whole = lax.all_gather(local.reshape(2, count, TILE_SIDE), "len", axis=1, tiled=True)
    return whole[0], whole[1]


def solution(mesh):
    return jax.shard_map(
        shards,
        mesh=mesh,
        in_specs=(P("tile"), P("len"), P("len"), P("tile", None)),
        out_specs=(P(None, "tile"), P(None, "tile")),
        check_vma=False,
    )
```

```python
import functools
import math

import jax
import jax.numpy as jnp
from jax import lax
from jax.experimental import pallas as pl
from jax.experimental.pallas import tpu as pltpu
from jax.sharding import PartitionSpec as P

MAX_LEN = 1024
TILE_SIDE = 512
EMPTY_VALUE = 2.0
VAR_EPS = 1e-05
MAX_EXCLUSION = 256
LANES = 128
CHUNK = 256
LOWEST = -3.0e38
WORD = 16
GROUP = 4


def round_up(value, multiple):
    return (value + multiple - 1) // multiple * multiple


def packed_piece(series, tile_list):
    piece_rows = -(-series.shape[0] // LANES)
    rows = round_up(piece_rows + 2, 8)
    values = jnp.pad(series, (0, piece_rows * LANES - series.shape[0])).reshape(piece_rows, LANES)
    slots = tile_list.T.astype(jnp.float32)
    slots = jnp.pad(slots, ((0, rows - piece_rows - 2), (0, LANES - slots.shape[1])), constant_values=-1.0)
    return jnp.concatenate([values, slots], axis=0)


def gather_pieces(piece, settings, count_tile):
    held = piece[None]
    mask = 1
    while True:
        other = lax.ppermute(held, "tile", [(b, b ^ mask) for b in range(count_tile)])
        mask *= 2
        if mask == count_tile:
            return held, other, settings
        held = jnp.concatenate([held, other], axis=0)
        if mask == 4:
            held, settings = lax.optimization_barrier((held, settings))


def flat_shift(values, amount):
    rows = values.shape[0]
    whole, part = divmod(amount, LANES)
    if whole:
        values = pltpu.roll(values, (rows - whole) % rows, 0)
    if part:
        rolled = pltpu.roll(values, LANES - part, 1)
        following = pltpu.roll(rolled, rows - 1, 0)
        lane = lax.broadcasted_iota(jnp.int32, values.shape, 1)
        values = jnp.where(lane < LANES - part, rolled, following)
    return values


def kernel(
    count_tile,
    count,
    piece_length,
    first_ref,
    second_ref,
    settings_ref,
    out_ref,
    slots_ref,
    flat_ref,
    centre_ref,
    inverse_ref,
    shifted_ref,
    turned_ref,
    left_ref,
    *rest,
):
    *right_refs, best_ref, number_ref, tile_ref = rest
    me = lax.axis_index("tile")
    half_slots = count_tile // 2
    piece_rows = -(-piece_length // LANES)
    series_rows = centre_ref.shape[1]
    blocks = TILE_SIDE // LANES
    square_row = lax.broadcasted_iota(jnp.int32, (LANES, LANES), 0)
    square_lane = lax.broadcasted_iota(jnp.int32, (LANES, LANES), 1)

    with jax.named_scope("numbers"):
        slots_ref[:half_slots] = first_ref[...]
        slots_ref[half_slots:] = second_ref[...]

        own_lane = lax.broadcasted_iota(jnp.int32, (1, count), 1)
        for kind in range(2):
            settings = settings_ref[kind : kind + 1, :].astype(jnp.float32)
            for index in range(count):
                number = jnp.sum(jnp.where(own_lane == index, settings, 0.0))
                number_ref[kind, index] = number.astype(jnp.int32)
        row_ids = slots_ref[:, piece_rows, :].astype(jnp.int32)
        col_ids = slots_ref[:, piece_rows + 1, :].astype(jnp.int32)
        near = (col_ids - row_ids) * TILE_SIDE - (TILE_SIDE - 1) <= MAX_EXCLUSION
        reach = (MAX_EXCLUSION + TILE_SIDE - 1) // TILE_SIDE

        def word_of(chosen, spot):
            chosen = chosen & (spot >= 0) & (spot < WORD)
            bit = jnp.left_shift(1, jnp.where(chosen, spot, 0)).astype(jnp.float32)
            return jnp.sum(jnp.where(chosen, bit, 0.0)).astype(jnp.int32)

        words = [
            [word_of((fixed == me) & ~near, listed - word * WORD) for word in range(-(-count_tile // WORD))]
            for fixed, listed in ((row_ids, col_ids), (col_ids, row_ids))
        ]
        around = jnp.where(row_ids == me, col_ids, row_ids) - me + reach
        near_word = word_of(((row_ids == me) | (col_ids == me)) & near, around)

    with jax.named_scope("list"):
        far_count = jnp.int32(0)
        for kind in range(2):
            for block in range(count_tile):
                tile_ref[0, far_count] = kind * count_tile + block
                word = words[kind][block // WORD]
                far_count = far_count + lax.bitwise_and(lax.shift_right_logical(word, block % WORD), 1)
        near_count = jnp.int32(0)
        for spot in range(2 * reach + 1):
            tile_ref[1, near_count] = me + spot - reach
            near_count = near_count + lax.bitwise_and(lax.shift_right_logical(near_word, spot), 1)

    with jax.named_scope("flat"):
        flat_ref[...] = jnp.zeros_like(flat_ref)
        lane = lax.broadcasted_iota(jnp.int32, (piece_rows, LANES), 1)
        for index in range(count_tile):
            piece = slots_ref[lax.bitwise_xor(me, index), :piece_rows, :]
            row, offset = divmod(index * piece_length, LANES)
            if offset:
                piece = pltpu.roll(piece, offset, 1)
                flat_ref[row + 1 : row + 1 + piece_rows] += jnp.where(lane < offset, piece, 0.0)
                piece = jnp.where(lane < offset, 0.0, piece)
            flat_ref[row : row + piece_rows] += piece

    inside = square_lane <= square_row

    def rotated(row):
        values = jnp.broadcast_to(flat_ref[row : row + 1, :], (LANES, LANES))
        return pltpu.roll(values, 1, 1, stride=1, stride_axis=0)

    def shift_rows(first, last):
        if first >= last:
            return
        current = rotated(first)
        for row in range(first, last):
            following = rotated(row + 1)
            shifted_ref[row] = jnp.where(inside, current, following)
            current = following

    with jax.named_scope("stats"):
        level_sum = flat_ref[:series_rows]
        level_square = jnp.zeros_like(level_sum)
        sums = [level_square] * count
        squares = [level_square] * count
        size = 1
        done = 0
        share = -(-(series_rows - 1) // MAX_LEN.bit_length())
        while True:
            for index in range(count):
                length = number_ref[0, index]
                taken = lax.bitwise_and(length, size) != 0
                tail = jnp.full((1, 1), lax.bitwise_and(length, size - 1), jnp.int32).astype(jnp.float32)
                tail_sum = flat_shift(sums[index], size)
                tail_square = flat_shift(squares[index], size)
                apart = tail_sum * (1.0 / jnp.maximum(tail, 1.0)) - level_sum * (1.0 / size)
                weight = tail * size / (tail + size)
                squares[index] = jnp.where(
                    taken, level_square + tail_square + apart * apart * weight, squares[index]
                )
                sums[index] = jnp.where(taken, level_sum + tail_sum, sums[index])
            shift_rows(done, min(done + share, series_rows - 1))
            done += share
            if size >= MAX_LEN:
                break
            next_sum = flat_shift(level_sum, size)
            next_square = flat_shift(level_square, size)
            apart = (next_sum - level_sum) * (1.0 / size)
            level_sum = level_sum + next_sum
            level_square = level_square + next_square + apart * apart * (size / 2)
            size *= 2
        for index in range(count):
            length = jnp.full((1, 1), number_ref[0, index], jnp.int32).astype(jnp.float32)
            centre_ref[index] = sums[index] / length
            inverse_ref[index] = 1.0 / jnp.sqrt(squares[index] / length + VAR_EPS)
        for spot in range(blocks + MAX_LEN // LANES - 1):
            turned_ref[spot] = shifted_ref[me * blocks + spot].T

    def per_length(index, carry):
        length = number_ref[0, index]
        barrier = number_ref[1, index]
        chunks = (length + CHUNK - 1) // CHUNK
        best_ref[index] = jnp.full_like(best_ref[index], LOWEST)
        best_ref[count + index] = jnp.full_like(best_ref[index], LOWEST)

        for steps in range(1, MAX_LEN // CHUNK + 1):
            depth = steps * CHUNK

            def build(operand_ref, other, chunk):
                for block in range(blocks):
                    row = other * blocks + block
                    centre = centre_ref[index, pl.ds(row, 1), :]
                    inverse = inverse_ref[index, pl.ds(row, 1), :]
                    for spot in range(chunk * CHUNK // LANES, (chunk + 1) * CHUNK // LANES):
                        values = (shifted_ref[row + spot] - centre) * inverse
                        operand_ref[
                            spot * LANES : (spot + 1) * LANES, block * LANES : (block + 1) * LANES
                        ] = values.astype(jnp.bfloat16)

            def product_with(operand_ref, other, steps=steps, build=build):
                product = None
                for chunk in range(steps):
                    part = slice(chunk * CHUNK, (chunk + 1) * CHUNK)
                    build(operand_ref, other, chunk)
                    term = jnp.dot(left_ref[:, part], operand_ref[part, :], preferred_element_type=jnp.float32)
                    product = term if product is None else product + term
                return product

            def improve(target, product):
                best = best_ref[target]
                for block in range(blocks):
                    best = jnp.maximum(best, product[:, block * LANES : (block + 1) * LANES])
                best_ref[target] = best

            @pl.when(chunks == steps)
            def _(depth=depth, product_with=product_with, improve=improve):
                with jax.named_scope(f"own{depth}"):
                    for block in range(blocks):
                        row = me * blocks + block
                        centre = jnp.broadcast_to(centre_ref[index, pl.ds(row, 1), :], (LANES, LANES)).T
                        inverse = jnp.broadcast_to(inverse_ref[index, pl.ds(row, 1), :], (LANES, LANES)).T
                        for spot in range(depth // LANES):
                            values = (turned_ref[block + spot] - centre) * inverse
                            if spot >= (depth - CHUNK) // LANES:
                                values = jnp.where(LANES - 1 - square_lane < length - spot * LANES, values, 0.0)
                            left_ref[
                                block * LANES : (block + 1) * LANES, spot * LANES : (spot + 1) * LANES
                            ] = values.astype(jnp.bfloat16)

                def near_tile(position, carry):
                    with jax.named_scope(f"near{depth}"):
                        other = tile_ref[1, position]
                        product = product_with(right_refs[0], other)
                        own_ids = lax.broadcasted_iota(jnp.int32, product.shape, 0)
                        other_ids = lax.broadcasted_iota(jnp.int32, product.shape, 1)
                        ahead = other_ids - own_ids
                        gap = (other - me) * TILE_SIDE
                        improve(index, jnp.where(ahead > barrier - gap, product, LOWEST))
                        improve(count + index, jnp.where(ahead < -barrier - gap, product, LOWEST))
                    return carry

                lax.fori_loop(0, near_count, near_tile, jnp.int32(0))

                def far_tiles(start, size):
                    with jax.named_scope(f"far{depth}x{size}"):
                        for step in range(size):
                            tile = tile_ref[0, start + step]
                            product = product_with(right_refs[step], lax.rem(tile, count_tile))
                            improve(tile // count_tile * count + index, product)

                def far_group(position, carry):
                    far_tiles(GROUP * position, GROUP)
                    return carry

                lax.fori_loop(0, far_count // GROUP, far_group, jnp.int32(0))
                size = GROUP // 2
                while size:

                    @pl.when(lax.bitwise_and(far_count, size) != 0)
                    def _(size=size):
                        far_tiles(far_count // (2 * size) * (2 * size), size)

                    size //= 2

        return carry

    lax.fori_loop(0, count, per_length, jnp.int32(0))

    with jax.named_scope("final"):
        for target in range(2 * count):
            length = jnp.full((1, 1), number_ref[0, target % count], jnp.int32).astype(jnp.float32)
            for block in range(blocks):
                best = best_ref[target, block * LANES : (block + 1) * LANES, :].T
                best = jnp.max(best, axis=0, keepdims=True)
                out_ref[target : target + 1, block * LANES : (block + 1) * LANES] = jnp.minimum(
                    1.0 - best / length, EMPTY_VALUE
                )


def local_profiles(first, second, settings, count_tile, piece_length):
    count = settings.shape[1]
    series_rows = round_up(count_tile * piece_length, 8 * LANES) // LANES
    vectors = [
        ((count_tile,) + first.shape[1:], jnp.float32),
        ((round_up(series_rows + first.shape[1], 8), LANES), jnp.float32),
        ((count, series_rows, LANES), jnp.float32),
        ((count, series_rows, LANES), jnp.float32),
        ((series_rows, LANES, LANES), jnp.float32),
        (((TILE_SIDE + MAX_LEN) // LANES - 1, LANES, LANES), jnp.float32),
        ((TILE_SIDE, MAX_LEN), jnp.bfloat16),
        *[((MAX_LEN, TILE_SIDE), jnp.bfloat16)] * GROUP,
        ((2 * count, TILE_SIDE, LANES), jnp.float32),
    ]
    used = sum(math.prod(shape) * jnp.dtype(kind).itemsize for shape, kind in vectors)
    return pl.pallas_call(
        functools.partial(kernel, count_tile, count, piece_length),
        out_shape=jax.ShapeDtypeStruct((2 * count, TILE_SIDE), jnp.float32),
        in_specs=[pl.BlockSpec(memory_space=pltpu.VMEM)] * 3,
        out_specs=pl.BlockSpec(memory_space=pltpu.VMEM),
        scratch_shapes=[pltpu.VMEM(shape, kind) for shape, kind in vectors]
        + [pltpu.SMEM((2, count), jnp.int32), pltpu.SMEM((2, 2 * count_tile + 1), jnp.int32)],
        compiler_params=pltpu.CompilerParams(vmem_limit_bytes=used + 8 * 2**20),
        name="profiles",
    )(first, second, settings)


def shards(series, window_lengths, exclusion, tile_list):
    count_tile, count_len = lax.axis_size("tile"), lax.axis_size("len")
    count = window_lengths.shape[0]
    piece = packed_piece(series, tile_list)
    settings = jnp.stack([window_lengths, exclusion])
    first, second, settings = gather_pieces(piece, settings, count_tile)
    local = local_profiles(first, second, settings, count_tile, series.shape[0])
    if count_len == 2:
        other = lax.ppermute(local, "len", [(0, 1), (1, 0)])
        swap = lax.axis_index("len") == 1
        low, high = jnp.where(swap, other, local), jnp.where(swap, local, other)
        whole = jnp.concatenate([low[:count], high[:count], low[count:], high[count:]], axis=0)
        whole = lax.optimization_barrier(whole)
        return whole[: 2 * count], whole[2 * count :]
    whole = lax.all_gather(local.reshape(2, count, TILE_SIDE), "len", axis=1, tiled=True)
    return whole[0], whole[1]


def solution(mesh):
    return jax.shard_map(
        shards,
        mesh=mesh,
        in_specs=(P("tile"), P("len"), P("len"), P("tile", None)),
        out_specs=(P(None, "tile"), P(None, "tile")),
        check_vma=False,
    )
```

```python
import functools
import math

import jax
import jax.numpy as jnp
from jax import lax
from jax.experimental import pallas as pl
from jax.experimental.pallas import tpu as pltpu
from jax.sharding import PartitionSpec as P

MAX_LEN = 1024
TILE_SIDE = 512
EMPTY_VALUE = 2.0
VAR_EPS = 1e-05
MAX_EXCLUSION = 256
LANES = 128
CHUNK = 256
LOWEST = -3.0e38
WORD = 16
assert MAX_EXCLUSION <= TILE_SIDE // 2
GROUP = 4


def round_up(value, multiple):
    return (value + multiple - 1) // multiple * multiple


def packed_piece(series, tile_list):
    piece_rows = -(-series.shape[0] // LANES)
    rows = round_up(piece_rows + 2, 8)
    values = jnp.pad(series, (0, piece_rows * LANES - series.shape[0])).reshape(piece_rows, LANES)
    slots = tile_list.T.astype(jnp.float32)
    slots = jnp.pad(slots, ((0, rows - piece_rows - 2), (0, LANES - slots.shape[1])), constant_values=-1.0)
    return jnp.concatenate([values, slots], axis=0)


def gather_pieces(piece, settings, count_tile):
    held = piece[None]
    mask = 1
    while True:
        other = lax.ppermute(held, "tile", [(b, b ^ mask) for b in range(count_tile)])
        mask *= 2
        if mask == count_tile:
            return held, other, settings
        held = jnp.concatenate([held, other], axis=0)
        if mask == 4:
            held, settings = lax.optimization_barrier((held, settings))


def flat_shift(values, amount):
    rows = values.shape[0]
    whole, part = divmod(amount, LANES)
    if whole:
        values = pltpu.roll(values, (rows - whole) % rows, 0)
    if part:
        rolled = pltpu.roll(values, LANES - part, 1)
        following = pltpu.roll(rolled, rows - 1, 0)
        lane = lax.broadcasted_iota(jnp.int32, values.shape, 1)
        values = jnp.where(lane < LANES - part, rolled, following)
    return values


def kernel(
    count_tile,
    count,
    piece_length,
    first_ref,
    second_ref,
    settings_ref,
    out_ref,
    slots_ref,
    flat_ref,
    centre_ref,
    inverse_ref,
    shifted_ref,
    turned_ref,
    left_ref,
    *rest,
):
    *right_refs, best_ref, number_ref, tile_ref = rest
    me = lax.axis_index("tile")
    half_slots = count_tile // 2
    piece_rows = -(-piece_length // LANES)
    series_rows = centre_ref.shape[1]
    blocks = TILE_SIDE // LANES
    square_row = lax.broadcasted_iota(jnp.int32, (LANES, LANES), 0)
    square_lane = lax.broadcasted_iota(jnp.int32, (LANES, LANES), 1)

    with jax.named_scope("numbers"):
        slots_ref[:half_slots] = first_ref[...]
        slots_ref[half_slots:] = second_ref[...]

        own_lane = lax.broadcasted_iota(jnp.int32, (1, count), 1)
        for kind in range(2):
            settings = settings_ref[kind : kind + 1, :].astype(jnp.float32)
            for index in range(count):
                number = jnp.sum(jnp.where(own_lane == index, settings, 0.0))
                number_ref[kind, index] = number.astype(jnp.int32)
        row_ids = slots_ref[:, piece_rows, :].astype(jnp.int32)
        col_ids = slots_ref[:, piece_rows + 1, :].astype(jnp.int32)
        near = col_ids - row_ids <= 1

        def word_of(chosen, spot):
            chosen = chosen & (spot >= 0) & (spot < WORD)
            bit = jnp.left_shift(1, jnp.where(chosen, spot, 0)).astype(jnp.float32)
            return jnp.sum(jnp.where(chosen, bit, 0.0)).astype(jnp.int32)

        words = [
            [word_of((fixed == me) & ~near, listed - word * WORD) for word in range(-(-count_tile // WORD))]
            for fixed, listed in ((row_ids, col_ids), (col_ids, row_ids))
        ]
        around = jnp.where(row_ids == me, col_ids, row_ids) - me + 1
        near_word = word_of(((row_ids == me) | (col_ids == me)) & near, around)

    with jax.named_scope("list"):
        far_count = jnp.int32(0)
        for kind in range(2):
            for block in range(count_tile):
                tile_ref[0, far_count] = kind * count_tile + block
                word = words[kind][block // WORD]
                far_count = far_count + lax.bitwise_and(lax.shift_right_logical(word, block % WORD), 1)
        side_count = jnp.int32(0)
        for spot in (0, 2):
            tile_ref[1, side_count] = me + spot - 1
            side_count = side_count + lax.bitwise_and(lax.shift_right_logical(near_word, spot), 1)
        diagonal = lax.bitwise_and(lax.shift_right_logical(near_word, 1), 1)

    with jax.named_scope("flat"):
        flat_ref[...] = jnp.zeros_like(flat_ref)
        lane = lax.broadcasted_iota(jnp.int32, (piece_rows, LANES), 1)
        for index in range(count_tile):
            piece = slots_ref[lax.bitwise_xor(me, index), :piece_rows, :]
            row, offset = divmod(index * piece_length, LANES)
            if offset:
                piece = pltpu.roll(piece, offset, 1)
                flat_ref[row + 1 : row + 1 + piece_rows] += jnp.where(lane < offset, piece, 0.0)
                piece = jnp.where(lane < offset, 0.0, piece)
            flat_ref[row : row + piece_rows] += piece

    inside = square_lane <= square_row
    ahead_square = square_lane - square_row

    def rotated(row):
        values = jnp.broadcast_to(flat_ref[row : row + 1, :], (LANES, LANES))
        return pltpu.roll(values, 1, 1, stride=1, stride_axis=0)

    def shift_rows(first, last):
        if first >= last:
            return
        current = rotated(first)
        for row in range(first, last):
            following = rotated(row + 1)
            shifted_ref[row] = jnp.where(inside, current, following)
            current = following

    with jax.named_scope("stats"):
        level_sum = flat_ref[:series_rows]
        level_square = jnp.zeros_like(level_sum)
        sums = [level_square] * count
        squares = [level_square] * count
        size = 1
        done = 0
        share = -(-(series_rows - 1) // MAX_LEN.bit_length())
        while True:
            for index in range(count):
                length = number_ref[0, index]
                taken = lax.bitwise_and(length, size) != 0
                tail = jnp.full((1, 1), lax.bitwise_and(length, size - 1), jnp.int32).astype(jnp.float32)
                tail_sum = flat_shift(sums[index], size)
                tail_square = flat_shift(squares[index], size)
                apart = tail_sum * (1.0 / jnp.maximum(tail, 1.0)) - level_sum * (1.0 / size)
                weight = tail * size / (tail + size)
                squares[index] = jnp.where(
                    taken, level_square + tail_square + apart * apart * weight, squares[index]
                )
                sums[index] = jnp.where(taken, level_sum + tail_sum, sums[index])
            shift_rows(done, min(done + share, series_rows - 1))
            done += share
            if size >= MAX_LEN:
                break
            next_sum = flat_shift(level_sum, size)
            next_square = flat_shift(level_square, size)
            apart = (next_sum - level_sum) * (1.0 / size)
            level_sum = level_sum + next_sum
            level_square = level_square + next_square + apart * apart * (size / 2)
            size *= 2
        for index in range(count):
            length = jnp.full((1, 1), number_ref[0, index], jnp.int32).astype(jnp.float32)
            centre_ref[index] = sums[index] / length
            inverse_ref[index] = 1.0 / jnp.sqrt(squares[index] / length + VAR_EPS)
        for spot in range(blocks + MAX_LEN // LANES - 1):
            turned_ref[spot] = shifted_ref[me * blocks + spot].T

    def per_length(index, carry):
        length = number_ref[0, index]
        barrier = number_ref[1, index]
        chunks = (length + CHUNK - 1) // CHUNK
        best_ref[index] = jnp.full_like(best_ref[index], LOWEST)
        best_ref[count + index] = jnp.full_like(best_ref[index], LOWEST)

        for steps in range(1, MAX_LEN // CHUNK + 1):
            depth = steps * CHUNK

            def build(operand_ref, other, chunk):
                for block in range(blocks):
                    row = other * blocks + block
                    centre = centre_ref[index, pl.ds(row, 1), :]
                    inverse = inverse_ref[index, pl.ds(row, 1), :]
                    for spot in range(chunk * CHUNK // LANES, (chunk + 1) * CHUNK // LANES):
                        values = (shifted_ref[row + spot] - centre) * inverse
                        operand_ref[
                            spot * LANES : (spot + 1) * LANES, block * LANES : (block + 1) * LANES
                        ] = values.astype(jnp.bfloat16)

            def product_with(operand_ref, other, steps=steps, build=build):
                product = None
                for chunk in range(steps):
                    part = slice(chunk * CHUNK, (chunk + 1) * CHUNK)
                    build(operand_ref, other, chunk)
                    term = jnp.dot(left_ref[:, part], operand_ref[part, :], preferred_element_type=jnp.float32)
                    product = term if product is None else product + term
                return product

            def improve(target, product):
                best = best_ref[target]
                for block in range(blocks):
                    best = jnp.maximum(best, product[:, block * LANES : (block + 1) * LANES])
                best_ref[target] = best

            @pl.when(chunks == steps)
            def _(depth=depth, product_with=product_with, improve=improve):
                with jax.named_scope(f"own{depth}"):
                    for block in range(blocks):
                        row = me * blocks + block
                        centre = jnp.broadcast_to(centre_ref[index, pl.ds(row, 1), :], (LANES, LANES)).T
                        inverse = jnp.broadcast_to(inverse_ref[index, pl.ds(row, 1), :], (LANES, LANES)).T
                        for spot in range(depth // LANES):
                            values = (turned_ref[block + spot] - centre) * inverse
                            if spot >= (depth - CHUNK) // LANES:
                                values = jnp.where(LANES - 1 - square_lane < length - spot * LANES, values, 0.0)
                            left_ref[
                                block * LANES : (block + 1) * LANES, spot * LANES : (spot + 1) * LANES
                            ] = values.astype(jnp.bfloat16)

                def side_tile(position, carry):
                    with jax.named_scope(f"side{depth}"):
                        other = tile_ref[1, position]
                        kind = jnp.where(other < me, 1, 0)
                        product = product_with(right_refs[0], other)
                        best = best_ref[kind * count + index]
                        rows = []
                        for high in range(blocks):
                            own = slice(high * LANES, (high + 1) * LANES)
                            row = best[own]
                            for wide in range(blocks):
                                part = product[own, wide * LANES : (wide + 1) * LANES]
                                ahead = ahead_square + (wide - high) * LANES
                                if (high - wide + 1) * LANES > TILE_SIDE - MAX_EXCLUSION:
                                    lowest = jnp.where(kind == 0, barrier - TILE_SIDE, -2 * TILE_SIDE)
                                    part = jnp.where(ahead > lowest, part, LOWEST)
                                if (wide - high + 1) * LANES > TILE_SIDE - MAX_EXCLUSION:
                                    highest = jnp.where(kind == 1, TILE_SIDE - barrier, 2 * TILE_SIDE)
                                    part = jnp.where(ahead < highest, part, LOWEST)
                                row = jnp.maximum(row, part)
                            rows.append(row)
                        best_ref[kind * count + index] = jnp.concatenate(rows, axis=0)
                    return carry

                lax.fori_loop(0, side_count, side_tile, jnp.int32(0))

                @pl.when(diagonal == 1)
                def _():
                    with jax.named_scope(f"diagonal{depth}"):
                        product = product_with(right_refs[0], me)
                        for kind in range(2):
                            for high in range(blocks):
                                own = slice(high * LANES, (high + 1) * LANES)
                                row = best_ref[kind * count + index, own, :]
                                for wide in range(high, blocks) if kind == 0 else range(high + 1):
                                    part = product[own, wide * LANES : (wide + 1) * LANES]
                                    ahead = ahead_square + (wide - high) * LANES
                                    if (abs(wide - high) - 1) * LANES < MAX_EXCLUSION:
                                        allowed = ahead > barrier if kind == 0 else ahead < -barrier
                                        part = jnp.where(allowed, part, LOWEST)
                                    row = jnp.maximum(row, part)
                                best_ref[kind * count + index, own, :] = row

                def far_tiles(start, size):
                    with jax.named_scope(f"far{depth}x{size}"):
                        for step in range(size):
                            tile = tile_ref[0, start + step]
                            product = product_with(right_refs[step], lax.rem(tile, count_tile))
                            improve(tile // count_tile * count + index, product)

                def far_group(position, carry):
                    far_tiles(GROUP * position, GROUP)
                    return carry

                lax.fori_loop(0, far_count // GROUP, far_group, jnp.int32(0))
                size = GROUP // 2
                while size:

                    @pl.when(lax.bitwise_and(far_count, size) != 0)
                    def _(size=size):
                        far_tiles(far_count // (2 * size) * (2 * size), size)

                    size //= 2

        return carry

    lax.fori_loop(0, count, per_length, jnp.int32(0))

    with jax.named_scope("final"):
        for target in range(2 * count):
            length = jnp.full((1, 1), number_ref[0, target % count], jnp.int32).astype(jnp.float32)
            for block in range(blocks):
                best = best_ref[target, block * LANES : (block + 1) * LANES, :].T
                best = jnp.max(best, axis=0, keepdims=True)
                out_ref[target : target + 1, block * LANES : (block + 1) * LANES] = jnp.minimum(
                    1.0 - best / length, EMPTY_VALUE
                )


def local_profiles(first, second, settings, count_tile, piece_length):
    count = settings.shape[1]
    series_rows = round_up(count_tile * piece_length, 8 * LANES) // LANES
    vectors = [
        ((count_tile,) + first.shape[1:], jnp.float32),
        ((round_up(series_rows + first.shape[1], 8), LANES), jnp.float32),
        ((count, series_rows, LANES), jnp.float32),
        ((count, series_rows, LANES), jnp.float32),
        ((series_rows, LANES, LANES), jnp.float32),
        (((TILE_SIDE + MAX_LEN) // LANES - 1, LANES, LANES), jnp.float32),
        ((TILE_SIDE, MAX_LEN), jnp.bfloat16),
        *[((MAX_LEN, TILE_SIDE), jnp.bfloat16)] * GROUP,
        ((2 * count, TILE_SIDE, LANES), jnp.float32),
    ]
    used = sum(math.prod(shape) * jnp.dtype(kind).itemsize for shape, kind in vectors)
    return pl.pallas_call(
        functools.partial(kernel, count_tile, count, piece_length),
        out_shape=jax.ShapeDtypeStruct((2 * count, TILE_SIDE), jnp.float32),
        in_specs=[pl.BlockSpec(memory_space=pltpu.VMEM)] * 3,
        out_specs=pl.BlockSpec(memory_space=pltpu.VMEM),
        scratch_shapes=[pltpu.VMEM(shape, kind) for shape, kind in vectors]
        + [pltpu.SMEM((2, count), jnp.int32), pltpu.SMEM((2, 2 * count_tile + 1), jnp.int32)],
        compiler_params=pltpu.CompilerParams(vmem_limit_bytes=used + 8 * 2**20),
        name="profiles",
    )(first, second, settings)


def shards(series, window_lengths, exclusion, tile_list):
    count_tile, count_len = lax.axis_size("tile"), lax.axis_size("len")
    count = window_lengths.shape[0]
    piece = packed_piece(series, tile_list)
    settings = jnp.stack([window_lengths, exclusion])
    first, second, settings = gather_pieces(piece, settings, count_tile)
    local = local_profiles(first, second, settings, count_tile, series.shape[0])
    if count_len == 2:
        other = lax.ppermute(local, "len", [(0, 1), (1, 0)])
        swap = lax.axis_index("len") == 1
        low, high = jnp.where(swap, other, local), jnp.where(swap, local, other)
        whole = jnp.concatenate([low[:count], high[:count], low[count:], high[count:]], axis=0)
        whole = lax.optimization_barrier(whole)
        return whole[: 2 * count], whole[2 * count :]
    whole = lax.all_gather(local.reshape(2, count, TILE_SIDE), "len", axis=1, tiled=True)
    return whole[0], whole[1]


def solution(mesh):
    return jax.shard_map(
        shards,
        mesh=mesh,
        in_specs=(P("tile"), P("len"), P("len"), P("tile", None)),
        out_specs=(P(None, "tile"), P(None, "tile")),
        check_vma=False,
    )
```
